128 devices in a mesh: blk: 32 (over x_hi, z, y), sub: 4 (over x_lo, core).
Axes of the slice: x: 4 (x_hi: 2, x_lo: 2; x = x_hi * 2 + x_lo), y: 4, z: 4, core: 2. Of those that a mesh axis runs over, the one named last changes fastest.
Arguments:
- integrals: float32 [32, 4, 32, 6144], P('blk', 'sub'), may hold values from -1 to 1
- slot_order: int32 [32, 4, 32], P('blk', 'sub'), may hold values from 0 to 31, each once within a row
- factor_rows: float32 [32, 4, 32, 4096], P(None, 'sub'), may hold values from -1 to 1.5, as said below
- occ_energy: float32 [384], replicated, may hold values from -1.5 to -0.3
- slab_index: int32 [1], replicated, may hold values from 0 to 127
- virt_energy: float32 [2048], replicated, may hold values from 0.1 to 3
Outputs:
- amplitudes: float32 [6144, 6144], P('blk', 'sub')
The draws below stay inside these ranges and needn't reach their ends.
Inputs may be any that keep to these rules, and one draw needn't show every extreme that they name: `slot_order`: each row of 32 entries holds every number from 0 to 31 once. `factor_rows`: the factor is lower triangular (zero above its diagonal) with diagonal entries between 0.5 and 1.5.
All inputs are finite; a program needn't handle non-finite values.
Results may differ from the reference program's by a relative error of at most 0.0001.
Values sent between devices are 32-bit elements; how exact they have to be, the bound alone decides.
No kernel may reach another device: no remote copies, remote signals or barrier semaphores. Data moves between devices by JAX's collectives and lax.ppermute only.
A program may use at most 128 MiB of HBM per device.

```python
import jax
import jax.numpy as jnp
from jax import lax

NAUX = 4096
NVIRT = 2048
NOCC = 3
NOCC_ALL = 384
PIECE = 32
ROUND = 128
ROUNDS = 32
PAIRS = 6144
N_SUB = 4


def draw_factor_rows(key, part):
    diag_key = jax.random.fold_in(key, 11)
    noise_key = jax.random.fold_in(key, 23)
    degrees = 2 * NAUX
    row_ids = jnp.arange(NAUX, dtype=jnp.int32)
    shapes = (degrees - row_ids).astype(jnp.float32) * 0.5
    chi_square = 2.0 * jax.random.gamma(diag_key, shapes, (NAUX,), jnp.float32)
    diagonal = jnp.sqrt(chi_square / jnp.float32(degrees))
    noise = jnp.clip(jax.random.normal(noise_key, (NAUX, NAUX), jnp.float32), -6.0, 6.0)
    row_scale = jnp.ones((NAUX,), jnp.float32)
    below = row_ids[:, None] > row_ids[None, :]
    on_diag = row_ids[:, None] == row_ids[None, :]
    off_part = noise / jnp.sqrt(jnp.float32(degrees))
    diag_part = jnp.clip(diagonal * row_scale, 0.5, 1.5)
    whole = jnp.where(below, off_part, 0.0)
    whole = jnp.where(on_diag, diag_part[:, None], whole)
    return whole.reshape(ROUNDS, ROUND // PIECE, PIECE, NAUX).astype(jnp.float32)


def block_levels(stream_key, shape, shards, low, high):
    def one(dim, blocks):
        steps = jax.random.uniform(jax.random.fold_in(jax.random.fold_in(stream_key, 6), dim), (blocks,), jnp.float32, low / len(shards), high / len(shards))
        return jnp.repeat(jnp.exp(steps), shape[dim] // blocks).reshape((-1,) + (1,) * (len(shape) - dim - 1))

    loudness = one(*shards[0])
    for cut in shards[1:]:
        loudness = loudness * one(*cut)
    return loudness


def centred(own_key, shape, deviation, most, split=(), kind=jnp.bfloat16):
    result = jax.random.normal(own_key, shape, jnp.float32) * deviation
    if len(split) > 0:
        result = block_levels(own_key, shape, split, -0.22, 0.18) * result
    return jnp.clip(result, min=-most, max=most).astype(kind)


def setup_inputs(seed: int = 0) -> dict:
    seeds = jax.random.split(jax.random.key(seed), 7)
    return {
        "integrals": centred(seeds[0], (ROUNDS, N_SUB, PIECE, PAIRS), 0.125, 1.0, ((0, 32), (1, 4)), jnp.float32),
        "slot_order": jax.vmap(lambda own: jax.random.permutation(own, PIECE))(jax.random.split(seeds[1], ROUNDS * N_SUB)).reshape((ROUNDS, N_SUB, PIECE)).astype(jnp.int32),
        "factor_rows": draw_factor_rows(jax.random.fold_in(seeds[6], 71), 0),
        "occ_energy": jnp.clip(jax.random.uniform(seeds[3], (NOCC_ALL,), jnp.float32, -1.5, -0.3), -1.5, -0.3),
        "slab_index": jax.random.randint(seeds[4], (1,), 0, NOCC_ALL // NOCC).astype(jnp.int32),
        "virt_energy": jnp.clip(jax.random.uniform(seeds[5], (NVIRT,), jnp.float32, 0.1, 3.0), 0.1, 3.0),
    }


PRECISE = lax.Precision.HIGHEST

def reference(integrals, slot_order, factor_rows, occ_energy, slab_index, virt_energy):
    piece_len = integrals.shape[2]
    places = jnp.arange(piece_len, dtype=jnp.int32)
    onehot = (slot_order[..., None] == places).astype(jnp.float32)
    canonical = jnp.einsum('rscq,rscp->rsqp', onehot, integrals.astype(jnp.float32), precision=PRECISE)
    right_side = canonical.reshape(NAUX, PAIRS)
    factor = factor_rows.reshape(NAUX, NAUX)
    fitted = jax.scipy.linalg.solve_triangular(factor, right_side, lower=True)
    coulomb = lax.dot_general(fitted, fitted, (((0,), (0,)), ((), ())), precision=PRECISE)
    slab_start = slab_index[0].astype(jnp.int32) * NOCC
    occ_slab = lax.dynamic_slice_in_dim(occ_energy, slab_start, NOCC)
    pair_energy = jnp.repeat(occ_slab, NVIRT) - jnp.tile(virt_energy, NOCC)
    return coulomb / (pair_energy[:, None] + pair_energy[None, :])
```

```python
import jax
import jax.numpy as jnp
from jax import lax
from jax.experimental import pallas as pl
from jax.experimental.pallas import tpu as pltpu
from jax.sharding import PartitionSpec as P

NVIRT = 2048
NOCC = 3
LANES = 128
HIGH = lax.Precision.HIGH

PART_XOR = (0, 2, 1, 3)
BAND = (0, 128, 384, 768)


def split_dot(left, right):
    left_hi = left.astype(jnp.bfloat16)
    left_lo = (left - left_hi.astype(jnp.float32)).astype(jnp.bfloat16)
    right_hi = right.astype(jnp.bfloat16)
    right_lo = (right - right_hi.astype(jnp.float32)).astype(jnp.bfloat16)

    def one(a, b):
        return jnp.dot(a, b, preferred_element_type=jnp.float32)

    return one(left_hi, right_hi) + (one(left_hi, right_lo) + one(left_lo, right_hi))


def invert_kernel(sub_ref, own_ref, x_ref, core_ref, both_ref, out_ref, block_ref):
    sub = sub_ref[0]
    for part_ref, flip in zip((own_ref, x_ref, core_ref, both_ref), PART_XOR):
        place = sub ^ flip
        for band in range(4):
            width = LANES * (band + 1)
            rows = pl.ds(pl.multiple_of(band * LANES + place * 32, 32), 32)
            block_ref[rows, 0:width] = part_ref[0, :, BAND[band] : BAND[band] + width]
    row = lax.broadcasted_iota(jnp.int32, (LANES, LANES), 0)
    col = lax.broadcasted_iota(jnp.int32, (LANES, LANES), 1)
    on_diag = row == col
    below = row > col

    def blk(i, j):
        return block_ref[i * LANES : (i + 1) * LANES, j * LANES : (j + 1) * LANES]

    tiles = [blk(i, i) for i in range(4)]
    inv = []
    for tile in tiles:
        kept = jnp.where(on_diag, tile, 0.0)
        down = 1.0 / jnp.sum(kept, axis=1, keepdims=True)
        across = 1.0 / jnp.sum(kept, axis=0, keepdims=True)
        pair = below & ((row ^ col) == 1)
        inv.append(jnp.where(on_diag, down, jnp.where(pair, -(tile * down) * across, 0.0)))
    for level in range(1, 7):
        mask = below & (((row >> level) ^ (col >> level)) == 1)
        inner = [split_dot(z, jnp.where(mask, tile, 0.0)) for z, tile in zip(inv, tiles)]
        inv = [z - split_dot(w, z) for z, w in zip(inv, inner)]
    full = {(i, i): inv[i] for i in range(4)}
    for i in (0, 2):
        full[i + 1, i] = -split_dot(split_dot(inv[i + 1], blk(i + 1, i)), inv[i])
    zero = jnp.zeros((LANES, LANES), jnp.float32)
    top = jnp.concatenate(
        [jnp.concatenate([inv[0], zero], 1), jnp.concatenate([full[1, 0], inv[1]], 1)], 0
    )
    low = jnp.concatenate(
        [jnp.concatenate([inv[2], zero], 1), jnp.concatenate([full[3, 2], inv[3]], 1)], 0
    )
    cross = -split_dot(split_dot(low, block_ref[256:512, 0:256]), top)
    for i in (2, 3):
        for j in (0, 1):
            full[i, j] = cross[(i - 2) * LANES : (i - 1) * LANES, j * LANES : (j + 1) * LANES]
    for i in range(4):
        for j in range(4):
            value = full[i, j].T if i >= j else zero
            for piece in range(4):
                flip = sub ^ piece
                part = ((flip & 1) << 1) | (flip >> 1)
                rows = pl.ds(pl.multiple_of(part * LANES + j * 32, 32), 32)
                out_ref[0, rows, i * LANES : (i + 1) * LANES] = value[piece * 32 : piece * 32 + 32]


def invert_blocks(sub, own, x_part, core_part, both_part):
    count = own.shape[0]
    spec = pl.BlockSpec((1, 32, 1280), lambda t, sub_ref: (t, 0, 0))
    return pl.pallas_call(
        invert_kernel,
        grid_spec=pltpu.PrefetchScalarGridSpec(
            num_scalar_prefetch=1,
            grid=(count,),
            in_specs=[spec] * 4,
            out_specs=pl.BlockSpec((1, 512, 512), lambda t, sub_ref: (t, 0, 0)),
            scratch_shapes=[pltpu.VMEM((512, 512), jnp.float32)],
        ),
        out_shape=jax.ShapeDtypeStruct((count, 512, 512), jnp.float32),
        name="invert_blocks",
    )(sub, own, x_part, core_part, both_part)


def order_kernel(slot_ref, in_ref, out_ref, row_ref):
    pieces, _, width = out_ref.shape
    for slot in range(in_ref.shape[0]):
        row_ref[pl.ds(slot_ref[slot], 1), :] = in_ref[slot : slot + 1, :]
    for piece in range(pieces):
        out_ref[piece] = row_ref[:, piece * width : (piece + 1) * width]


def canonical_pieces(slot_order, integrals, pieces):
    slots, pairs = integrals.shape
    return pl.pallas_call(
        order_kernel,
        in_specs=[
            pl.BlockSpec(memory_space=pltpu.SMEM),
            pl.BlockSpec(memory_space=pltpu.VMEM),
        ],
        out_specs=pl.BlockSpec(memory_space=pltpu.VMEM),
        scratch_shapes=[pltpu.VMEM((slots, pairs), jnp.float32)],
        out_shape=jax.ShapeDtypeStruct((pieces, slots, pairs // pieces), jnp.float32),
        name="canonical_pieces",
    )(slot_order, integrals)


def over_sub(value, flip):
    return lax.ppermute(value, "sub", [(s, s ^ flip) for s in range(4)])


def over_blk(value, flip):
    return lax.ppermute(value, "blk", [(b, b ^ flip) for b in range(32)])


def over_far_x(value):
    pairs = [(b * 4 + s, (b ^ 16) * 4 + (s ^ 2)) for b in range(32) for s in range(4)]
    return lax.ppermute(value, ("blk", "sub"), pairs)


def over_middle_x(value):
    pairs = []
    for b in range(32):
        for s in range(4):
            other = (b ^ 16, s ^ 2) if (b >> 4) != (s >> 1) else (b, s)
            pairs.append((b * 4 + s, other[0] * 4 + other[1]))
    return lax.ppermute(value, ("blk", "sub"), pairs)


def dot_nt(left, right):
    return lax.dot_general(left, right, (((1,), (1,)), ((), ())), precision=HIGH)


CHUNKS = ((0, 1, 2), (3, 4, 5), (6, 7))


def shards(integrals, slot_order, factor_rows, occ_energy, slab_index, virt_energy):
    blk = lax.axis_index("blk")
    sub = lax.axis_index("sub")
    own_rows = factor_rows.reshape(1024, 4096)

    packed = jnp.stack(
        [
            jnp.concatenate(
                [
                    own_rows[
                        t * 128 + band * 32 : t * 128 + band * 32 + 32,
                        t * 512 : t * 512 + 128 * (band + 1),
                    ]
                    for band in range(4)
                ],
                1,
            )
            for t in range(8)
        ]
    )
    half_a, half_b = packed[:4], packed[4:]
    x_a = over_sub(half_a, 2)
    x_b = over_far_x(half_b)
    core_a, core_b = over_sub(half_a, 1), over_sub(half_b, 1)
    pieces = canonical_pieces(
        slot_order.reshape(32), integrals.reshape(32, 6144), 32
    )
    arrived = lax.all_to_all(pieces, "blk", 0, 0, tiled=True)
    rhs = arrived.reshape(1024, 192).T
    both_a, both_b = over_sub(x_a, 1), over_sub(x_b, 1)
    sub_arg = sub.astype(jnp.int32).reshape(1)
    inverse_a = invert_blocks(sub_arg, half_a, x_a, core_a, both_a)
    inverse_b = invert_blocks(sub_arg, half_b, x_b, core_b, both_b)
    inverses = [inverse_a[t] for t in range(4)] + [inverse_b[t] for t in range(4)]

    core = sub & 1
    x_lo = sub >> 1
    y_bit0 = blk & 1
    z_pos = (blk >> 2) & 3

    current = rhs[:, :128]
    rest = rhs[:, 128:]
    halves = []
    tile = None
    chunk_ends = {chunk[-1]: chunk for chunk in CHUNKS}
    for t in range(8):
        from_x = over_sub(current, 2)
        two = jnp.concatenate([current, from_x], 1)
        from_core = over_sub(two, 1)
        whole = jnp.concatenate([two, from_core], 1)
        solved = jnp.dot(whole, inverses[t], precision=HIGH)
        cols = slice(t * 512, t * 512 + 512)
        if t < 7:
            current = rest[:, :128] - dot_nt(solved, own_rows[t * 128 + 128 : t * 128 + 256, cols])
        if t < 6:
            rest = rest[:, 128:] - dot_nt(solved, own_rows[t * 128 + 256 :, cols])
        halves.append(jnp.where(core == 0, solved[:, :256], solved[:, 256:]))
        if t in chunk_ends:
            own = jnp.concatenate([halves[i] for i in chunk_ends[t]], 1)
            side = over_middle_x(own)
            left = jnp.concatenate([own] + [over_blk(own, k) for k in (1, 2, 3)], 0)
            right = jnp.concatenate([side] + [over_blk(side, 4 * k) for k in (1, 2, 3)], 0)
            part = dot_nt(left, right)
            tile = part if tile is None else tile + part

    same = (z_pos >> 1) == core
    kept = jnp.where(same, tile[:, :384], tile[:, 384:])
    sent = jnp.where(same, tile[:, 384:], tile[:, :384])
    summed = kept + over_sub(sent, 1)
    rows = [summed[:192]] + [over_blk(summed[192 * k : 192 * k + 192], k) for k in (1, 2, 3)]
    cells = jnp.stack(rows).reshape(4, 192, 2, 192).transpose(2, 0, 1, 3)
    cells = jnp.where((z_pos & 1) == 1, cells[::-1], cells)
    cells = cells.reshape(2, 2, 2, 192, 192)
    cells = jnp.where((blk & 2) == 2, cells[:, ::-1], cells)
    cells = jnp.where((blk & 1) == 1, cells[:, :, ::-1], cells)
    coulomb = cells.reshape(8, 192, 192).transpose(1, 0, 2).reshape(192, 1536)

    slab_start = slab_index[0] * NOCC
    occ_slab = lax.dynamic_slice_in_dim(occ_energy, slab_start, NOCC)
    pair_energy = jnp.repeat(occ_slab, NVIRT) - jnp.tile(virt_energy, NOCC)
    row_energy = lax.dynamic_slice_in_dim(pair_energy, blk * 192, 192)
    col_energy = lax.dynamic_slice_in_dim(pair_energy, sub * 1536, 1536)
    return coulomb / (row_energy[:, None] + col_energy[None, :])


def solution(mesh):
    in_specs = (
        P("blk", "sub", None, None),
        P("blk", "sub", None),
        P(None, "sub", None, None),
        P(),
        P(),
        P(),
    )
    out_specs = P("blk", "sub")
    return jax.shard_map(shards, mesh=mesh, in_specs=in_specs, out_specs=out_specs, check_vma=False)
```
